512 devices in a mesh: groups: 2 (over y), aa: 32 (over z), ba: 4 (over x), col: 2 (over core).
Axes of the slice: x: 4, y: 2, z: 32, core: 2. Of those that a mesh axis runs over, the one named last changes fastest.
The devices are a block of a 4x8x32 slice.
Arguments:
- hidden: bfloat16 [256, 128, 8192], P(('groups', 'aa'), None, ('ba', 'col')), parts along dimension 0, may hold values from -6 to 6
- key_value_weight: bfloat16 [2048, 8192], P('aa', ('ba', 'col')), may hold values from -0.125 to 0.125
- adapter_down_weight: bfloat16 [256, 32, 8192], P(('groups', 'aa'), None, ('ba', 'col')), parts along dimension 0, may hold values from -0.0625 to 0.0625
- adapter_up_weight: bfloat16 [256, 16, 2048], P(('groups', 'aa'), None, ('ba', 'col')), parts along dimension 0, may hold values from -1.5 to 1.5
- prompt_block_count: int32 [128], P('groups'), parts along dimension 0, may hold values from 1 to 3, 128 in all
- request_adapter: int32 [128], P('groups'), parts along dimension 0, may hold values from 0 to 127
- adapter_bank_row: int32 [256], P('groups'), parts along dimension 0, may hold values from 0 to 127, each once
Outputs:
- kv_states: bfloat16 [256, 128, 2048], P(('groups', 'aa'), None, ('ba', 'col')), parts along dimension 0
The draws below stay inside these ranges and needn't reach their ends.
There are 2 independent parts, one for each index of `groups`. The reference program is written for one: setup_inputs(seed, part) draws one part's arguments, and reference() takes and returns one part's arrays. A program takes and returns all parts, laid end to end along the dimension named above; an argument that names none is the same for every part. Nothing has to cross between parts.
Inputs may be any that keep to these rules, and one draw needn't show every extreme that they name: prompt_block_count sum to 128; some request has exactly 3 blocks. `adapter_bank_row`: each bank row holds one adapter; bank row s lies on index s // 4 of aa.
All inputs are finite; a program needn't handle non-finite values.
Results may differ from the reference program's by a relative error of at most 0.001.
Values may be sent and summed in bfloat16 or wider, within the bound.
No kernel may reach another device: no remote copies, remote signals or barrier semaphores. Data moves between devices by JAX's collectives and lax.ppermute only.
A program may use at most 128 MiB of HBM per device.

```python
import math
import jax
import jax.numpy as jnp
import numpy as np
from jax import lax

MODEL_WIDTH = 8192
ADAPTER_RANK = 16
BLOCK = 128
MOSTC = 3
KEY_VALUE_WIDTH = 1024
BLOCKS = 128
REQS = 64
ADAPTER_COUNT = 128


def with_ends(array, key, smallest, top_value):
    shape = array.shape
    place = [jax.random.randint(jax.random.fold_in(key, axis), (), 0, shape[axis]) for axis in range(len(shape))]
    array = array.at[tuple(place)].set(smallest)
    longest = shape.index(max(shape))
    place[longest] = (place[longest] + 1) % shape[longest]
    return array.at[tuple(place)].set(top_value)


def with_spikes(entries, key, source, target, parts, factor):
    owner, partner = [(jnp.arange(entries.shape[axis_at]) // (entries.shape[axis_at] // parts)).reshape([-1 if axis == axis_at else 1 for axis in range(entries.ndim)]) for axis_at in (source, target)]
    chosen = jax.random.permutation(key, parts)[partner]
    strong = (owner == chosen) | (owner == (partner + parts // 2) % parts)
    return jnp.where(strong, factor * entries, entries)


def steps_of(own_key, shape, shards, low, top_value):
    loudness, own = 1.0, jax.random.fold_in(own_key, 6)
    for axis_at, parts in shards:
        heights = jnp.exp(jax.random.uniform(jax.random.fold_in(own, axis_at), (parts,), jnp.float32, low / len(shards), top_value / len(shards)))
        loudness = loudness * jnp.repeat(heights, shape[axis_at] // parts).reshape([-1 if axis == axis_at else 1 for axis in range(len(shape))])
    return loudness


def rank_table(count, skew):
    weights = [(1 << 20) // math.isqrt(standing ** skew) + 1 for standing in range(1, count + 1)]
    scale = 1 + sum(weights) // (1 << 30)
    return np.cumsum(np.array([max(1, weight // scale) for weight in weights]))


def ranked(stream_key, shape, count, skew):
    grid = rank_table(count, skew)
    lot = jax.random.randint(jax.random.fold_in(stream_key, 1), shape, 0, int(grid[count - 1]))
    standing = jnp.searchsorted(jnp.asarray(grid, jnp.int32), lot, side="right")
    return jax.random.permutation(jax.random.fold_in(stream_key, 2), count)[standing].astype(jnp.int32)


def length_profile(number_of, total, reach, lean):
    portions = [(1 << 20) // math.isqrt(standing ** lean) + 1 for standing in range(2, number_of + 1)]
    spare, holding = total - reach - (number_of - 1), [1] * (number_of - 1)
    while spare > 0:
        movable = [i for i in range(number_of - 1) if holding[i] < reach]
        pool, budget = sum([portions[i] for i in movable]), spare
        for i in movable:
            addition = min(reach - holding[i], max(1, budget * portions[i] // pool), spare)
            holding[i] = holding[i] + addition
            spare = spare - addition
    return np.array([reach] + holding)


def uneven(rng, count, total, bound, skew):
    if count == 2:
        one = jax.random.randint(rng, (), max(1, total - bound), min(bound, total - 1) + 1)
        return jnp.stack([one, total - one])
    lengths = jnp.asarray(length_profile(count, total, bound, skew), jnp.int32)
    pairs = (count - 1) // 2
    source_of, taker = lengths[1:1 + 2 * pairs:2], lengths[2:2 + 2 * pairs:2]
    slack = jnp.minimum(source_of - 1, bound - taker)
    shifted = jax.random.randint(jax.random.fold_in(rng, 1), (pairs,), 0, 1 << 20) % (slack + 1)
    lengths = lengths.at[1:1 + 2 * pairs:2].set(source_of - shifted).at[2:2 + 2 * pairs:2].set(taker + shifted)
    return lengths[jax.random.permutation(jax.random.fold_in(rng, 2), count)]


def scatter_about(key, extent, scale, most, shards=(), kind=jnp.bfloat16):
    entries = scale * jax.random.normal(key, extent, jnp.float32)
    if shards:
        entries = entries * steps_of(key, extent, shards, -0.22, 0.18)
    return jnp.clip(entries, -most, most).astype(kind)


def noise_with(stream_key, shape, scale, limit, pieces, heavy, kind=jnp.bfloat16):
    entries = scale * jax.random.normal(stream_key, shape, jnp.float32)
    if pieces:
        entries = entries * steps_of(stream_key, shape, pieces, -0.22, 0.18)
    return jnp.clip(with_spikes(entries, jax.random.fold_in(stream_key, 3), *heavy), -limit, limit).astype(kind)


def setup_inputs(seed: int = 0, part: int = 0) -> dict:
    seeds = jax.random.split(jax.random.key(seed), 8)
    part_keys = jax.random.split(jax.random.fold_in(seeds[7], part), 8)
    hidden = scatter_about(part_keys[0], (BLOCKS, BLOCK, MODEL_WIDTH), 1.0, 6.0, ((0, 32), (2, 8)))
    key_value_weight = noise_with(seeds[1], (2 * KEY_VALUE_WIDTH, MODEL_WIDTH), MODEL_WIDTH ** -0.5, 0.125, ((0, 32), (1, 8)), (1, 0, 32, 2.75))
    adapter_down_weight = scatter_about(part_keys[2], (ADAPTER_COUNT, 2 * ADAPTER_RANK, MODEL_WIDTH), MODEL_WIDTH ** -0.5, 0.0625, ((0, 32), (2, 8)))
    adapter_up_weight = scatter_about(part_keys[3], (ADAPTER_COUNT, ADAPTER_RANK, 2 * KEY_VALUE_WIDTH), ADAPTER_RANK ** -0.5, 1.5, ((0, 32), (2, 8)))
    prompt_block_count = uneven(part_keys[4], REQS, BLOCKS, MOSTC, 2).astype(jnp.int32)
    request_adapter = with_ends(ranked(part_keys[5], (REQS,), ADAPTER_COUNT, 2), jax.random.fold_in(part_keys[5], 3), 0, ADAPTER_COUNT - 1).astype(jnp.int32)
    adapter_bank_row = jax.random.permutation(part_keys[6], ADAPTER_COUNT).astype(jnp.int32)
    return dict(hidden=hidden, key_value_weight=key_value_weight, adapter_down_weight=adapter_down_weight, adapter_up_weight=adapter_up_weight, prompt_block_count=prompt_block_count, request_adapter=request_adapter, adapter_bank_row=adapter_bank_row)


def block_slots(prompt_block_count, request_adapter, adapter_bank_row):
    block_ids = jnp.arange(BLOCKS, dtype=jnp.int32)
    block_ends = jnp.cumsum(prompt_block_count).astype(jnp.int32)
    request_of = jnp.sum((block_ends[None, :] <= block_ids[:, None]).astype(jnp.int32), axis=1).astype(jnp.int32)
    request_ids = jnp.arange(REQS, dtype=jnp.int32)
    adapter_of = jnp.sum(jnp.where(request_of[:, None] == request_ids[None, :], request_adapter[None, :], 0), axis=1).astype(jnp.int32)
    adapter_rows = jnp.arange(ADAPTER_COUNT, dtype=jnp.int32)
    return jnp.sum(jnp.where(adapter_of[:, None] == adapter_rows[None, :], adapter_bank_row[None, :], 0), axis=1).astype(jnp.int32)


def reference(hidden, key_value_weight, adapter_down_weight, adapter_up_weight, prompt_block_count, request_adapter, adapter_bank_row):
    bank_row_lookup = block_slots(prompt_block_count, request_adapter, adapter_bank_row)
    token_rows = hidden.reshape(BLOCKS * BLOCK, MODEL_WIDTH)
    base_output = lax.dot_general(token_rows, key_value_weight, (((1,), (1,)), ((), ())), preferred_element_type=jnp.float32)
    base_output = base_output.reshape(BLOCKS, BLOCK, 2 * KEY_VALUE_WIDTH)

    def single_block(operands):
        block_rows, current_bank_row = operands
        current_down_weight = lax.dynamic_index_in_dim(adapter_down_weight, current_bank_row, 0, keepdims=False)
        current_up_weight = lax.dynamic_index_in_dim(adapter_up_weight, current_bank_row, 0, keepdims=False).astype(jnp.float32)
        low_rank = lax.dot_general(block_rows, current_down_weight, (((1,), (1,)), ((), ())), preferred_element_type=jnp.float32)
        key_part = jnp.dot(low_rank[:, :ADAPTER_RANK], current_up_weight[:, :KEY_VALUE_WIDTH], precision=lax.Precision.HIGHEST)
        value_part = jnp.dot(low_rank[:, ADAPTER_RANK:], current_up_weight[:, KEY_VALUE_WIDTH:], precision=lax.Precision.HIGHEST)
        return jnp.concatenate([key_part, value_part], axis=1)

    adapter_output = lax.map(single_block, (hidden, bank_row_lookup))
    return (base_output + adapter_output).astype(jnp.bfloat16)
```

```python
import jax
import jax.numpy as jnp
from jax import lax
from jax.sharding import Mesh
from jax.sharding import PartitionSpec as P


AA = ("ah", "al")
LANES = ("ba", "col")
SWAP = [(0, 1), (1, 0)]


def block_slots(prompt_block_count, request_adapter, adapter_bank_row, block_total):
    block_ids = jnp.arange(block_total, dtype=jnp.int32)
    requests = prompt_block_count.shape[0]
    earlier = jnp.arange(requests)[:, None] >= jnp.arange(requests)[None, :]
    block_ends = jnp.sum(jnp.where(earlier, prompt_block_count[None, :], 0), axis=1)
    request_of = jnp.sum((block_ends[None, :] <= block_ids[:, None]).astype(jnp.int32), axis=1)
    request_ids = jnp.arange(requests, dtype=jnp.int32)
    adapter_of = jnp.sum(
        jnp.where(request_of[:, None] == request_ids[None, :], request_adapter[None, :], 0), axis=1
    )
    adapter_rows = jnp.arange(adapter_bank_row.shape[0], dtype=jnp.int32)
    return jnp.sum(
        jnp.where(adapter_of[:, None] == adapter_rows[None, :], adapter_bank_row[None, :], 0),
        axis=1,
    )


def low_rank_term(hidden, down, up, slots):
    blocks, _, width = hidden.shape
    owned, ranks, _ = down.shape
    half_ranks, span = up.shape[1:]
    owners = lax.axis_size(AA)
    rest = half_ranks * span // ranks
    rows = jnp.concatenate([down, up.reshape(owned, ranks, rest)], axis=2)
    per = ranks // owners
    pieces = rows.reshape(owned, owners, per * (width + rest)).transpose(1, 0, 2)
    held = lax.all_to_all(pieces, AA, 0, 0, tiled=True).reshape(owners * owned, -1)
    bank_rows = jnp.arange(owners * owned, dtype=jnp.int32)
    chosen = (slots[:, None] == bank_rows[None, :]).astype(held.dtype)
    wanted = jnp.dot(chosen, held, preferred_element_type=jnp.float32).astype(held.dtype)
    mine = lax.all_to_all(wanted.reshape(owners, blocks, -1), AA, 0, 0, tiled=True)
    mine = mine.transpose(1, 0, 2).reshape(blocks, ranks, width + rest)
    down_rows = mine[:, :, :width]
    up_rows = mine[:, :, width:].reshape(blocks, half_ranks, span).astype(jnp.float32)
    low = jnp.einsum("ckf,ctf->ckt", down_rows, hidden, preferred_element_type=jnp.float32)
    lanes = lax.axis_size(LANES)
    keys, values = low[:, :half_ranks], low[:, half_ranks:]
    dealt = jnp.concatenate(
        [jnp.broadcast_to(x, (lanes // 2, *x.shape)) for x in (keys, values)], axis=0
    )
    active = lax.all_to_all(dealt, LANES, 0, 0, tiled=True).sum(axis=0)
    return jnp.einsum("ckt,ckj->ctj", active, up_rows, precision=lax.Precision.HIGHEST)


def body(
    hidden,
    key_value_weight,
    adapter_down_weight,
    adapter_up_weight,
    prompt_block_count,
    request_adapter,
    adapter_bank_row,
):
    blocks, block_len, width = hidden.shape
    tokens = blocks * block_len
    owners = lax.axis_size(AA)
    ring = lax.axis_size("ba")
    parity = lax.axis_index("al")
    place = lax.axis_index("ba")
    core = lax.axis_index("col")

    rows = key_value_weight.shape[0]
    half = rows // 2
    kept = lax.dynamic_slice_in_dim(key_value_weight, core * half, half)
    given = lax.dynamic_slice_in_dim(key_value_weight, (1 - core) * half, half)
    weight = jnp.concatenate([kept, lax.ppermute(given, "col", SWAP)], axis=1)
    weight = lax.all_gather(weight, "ah", axis=0, tiled=True)

    token_rows = hidden.reshape(tokens, width)
    pair_rows = jnp.concatenate([token_rows, lax.ppermute(token_rows, "al", SWAP)], axis=0)
    pair_rows = jnp.concatenate([pair_rows, lax.ppermute(pair_rows, "col", SWAP)], axis=1)

    slots = block_slots(
        prompt_block_count, request_adapter, adapter_bank_row, blocks * owners
    )
    adapted = low_rank_term(hidden, adapter_down_weight, adapter_up_weight, slots)

    lane_rows = weight.shape[0] // (2 * ring)

    def product(target):
        first = (2 * lax.rem(target + 2 * ring, ring)) * lane_rows
        ours = lax.dynamic_slice_in_dim(weight, first + core * lane_rows, lane_rows)
        theirs = lax.dynamic_slice_in_dim(weight, first + (1 - core) * lane_rows, lane_rows)
        return lax.dot_general(
            pair_rows,
            jnp.concatenate([ours, theirs], axis=0),
            (((1,), (1,)), ((), ())),
            preferred_element_type=jnp.float32,
        )

    ahead = [(2 * i + c, 2 * ((i + 1 - 2 * c) % ring) + c) for i in range(ring) for c in range(2)]
    behind = [(2 * i + c, 2 * ((i - 1 + 2 * c) % ring) + c) for i in range(ring) for c in range(2)]
    turn = 1 - 2 * core
    far = lax.ppermute(product(place + 2), LANES, ahead)
    other = lax.ppermute(product(place - turn), LANES, behind)
    near = lax.ppermute(product(place + turn) + far, LANES, ahead)
    total = product(place) + near + other

    crossed = lax.ppermute(total[tokens:], "al", SWAP)
    both = jnp.stack([total[:tokens], crossed])
    here = both[:, :, :lane_rows]
    there = lax.ppermute(both[:, :, lane_rows:], "col", SWAP)
    even = jnp.where(parity == 0, 0, 1)
    first_half = [jnp.where(core == 0, here, there), jnp.where(core == 0, there, here)]
    columns = []
    for source in range(lane_rows // half):
        for odd in range(2):
            for piece in first_half:
                part = piece[:, :, source * half : (source + 1) * half]
                columns.append(jnp.where(even == odd, part[0], part[1]))
    base = jnp.concatenate(columns, axis=1).reshape(blocks, block_len, -1)
    return (base + adapted).astype(jnp.bfloat16)


def solution(mesh):
    groups, owners, ring, cores = (mesh.shape[a] for a in ("groups", "aa", "ba", "col"))
    split = Mesh(
        mesh.devices.reshape(groups, owners // 2, 2, ring, cores),
        ("groups", "ah", "al", "ba", "col"),
    )
    rows = ("groups", *AA)
    placed = (
        P(rows, None, LANES),
        P(AA, LANES),
        P(rows, None, LANES),
        P(rows, None, LANES),
        P("groups"),
        P("groups"),
        P("groups"),
    )
    return jax.shard_map(
        body,
        mesh=split,
        in_specs=placed,
        out_specs=P(rows, None, LANES),
        check_vma=False,
    )
```

```python
import jax
import jax.numpy as jnp
from jax import lax
from jax.sharding import Mesh
from jax.sharding import PartitionSpec as P


AA = ("ah", "al")
LANES = ("ba", "col")
SWAP = [(0, 1), (1, 0)]


def block_slots(prompt_block_count, request_adapter, adapter_bank_row, block_total):
    block_ids = jnp.arange(block_total, dtype=jnp.int32)
    requests = prompt_block_count.shape[0]
    earlier = jnp.arange(requests)[:, None] >= jnp.arange(requests)[None, :]
    block_ends = jnp.sum(jnp.where(earlier, prompt_block_count[None, :], 0), axis=1)
    request_of = jnp.sum((block_ends[None, :] <= block_ids[:, None]).astype(jnp.int32), axis=1)
    request_ids = jnp.arange(requests, dtype=jnp.int32)
    adapter_of = jnp.sum(
        jnp.where(request_of[:, None] == request_ids[None, :], request_adapter[None, :], 0), axis=1
    )
    adapter_rows = jnp.arange(adapter_bank_row.shape[0], dtype=jnp.int32)
    return jnp.sum(
        jnp.where(adapter_of[:, None] == adapter_rows[None, :], adapter_bank_row[None, :], 0),
        axis=1,
    )


def exchange(x, axis):
    owners = lax.axis_size(AA)
    up = [(i, (i + 1) % owners) for i in range(owners)]
    down = [(i, (i - 1) % owners) for i in range(owners)]
    first, second = jnp.split(x, 2, axis=axis)
    ways = (up, down) if axis == 0 else (down, up)
    first, second = lax.ppermute(first, AA, ways[0]), lax.ppermute(second, AA, ways[1])
    return jnp.concatenate([first, second], axis=axis)


def across(x):
    owners = lax.axis_size("ah")
    odd = [2 * i + 1 for i in range(owners)]
    even = [2 * ((i + 1) % owners) for i in range(owners)]
    return lax.ppermute(x, AA, [*zip(odd, even), *zip(even, odd)])


def deal_rows(down, up):
    owned, ranks, width = down.shape
    span = up.shape[2]
    halves = ranks // 2
    rest = up.shape[1] * span // ranks
    parity = lax.axis_index("al")
    rows = jnp.concatenate([down, up.reshape(owned, ranks, rest)], axis=2)
    rows = rows.reshape(owned, 2, halves, width + rest)
    kept = lax.dynamic_index_in_dim(rows, parity, 1, keepdims=False)
    given = lax.dynamic_index_in_dim(rows, 1 - parity, 1, keepdims=False)
    rows = jnp.concatenate([kept, across(given)], axis=0)
    owners = lax.axis_size("ah")
    pieces = rows.reshape(2 * owned, owners, -1).transpose(1, 0, 2)
    return lax.all_to_all(pieces, "ah", 0, 0, tiled=True).reshape(owners * 2 * owned, -1)


def choose_rows(held, slots, owned):
    parity = lax.axis_index("al")
    owners = lax.axis_size("ah")
    owner, inside = slots // owned, slots % owned
    step = 1 - 2 * parity
    matching = owner % 2 == parity
    holder = jnp.where(matching, owner // 2, ((owner + step) % (2 * owners)) // 2)
    place = holder * (2 * owned) + jnp.where(matching, inside, inside + owned)
    by_owner = place.reshape(owners, 2, -1)
    own = jnp.where(parity == 0, by_owner[:, 0], by_owner[:, 1])
    other = jnp.where(
        parity == 0, jnp.roll(by_owner[:, 1], 1, axis=0), jnp.roll(by_owner[:, 0], -1, axis=0)
    )
    place = jnp.concatenate([own, other], axis=1).reshape(-1)
    rows = jnp.arange(held.shape[0], dtype=jnp.int32)
    chosen = (place[:, None] == rows[None, :]).astype(held.dtype)
    return jnp.dot(chosen, held, preferred_element_type=jnp.float32).astype(held.dtype)


def own_rows(wanted, blocks, ranks, width):
    parity = lax.axis_index("al")
    owners = lax.axis_size("ah")
    pieces = lax.all_to_all(wanted.reshape(owners, 2 * blocks, -1), "ah", 0, 0, tiled=True)
    kept, taken = pieces[:, :blocks], across(pieces[:, blocks:])
    first = jnp.where(parity == 0, kept, taken)
    second = jnp.where(parity == 0, taken, kept)
    rows = jnp.concatenate([first, second], axis=0).transpose(1, 0, 2)
    rows = rows.reshape(blocks, ranks, -1)
    return rows[:, :, :width], rows[:, :, width:].reshape(blocks, ranks // 2, -1)


def over_lanes(low):
    half_ranks = low.shape[1] // 2
    lanes = lax.axis_size(LANES)
    keys, values = low[:, :half_ranks], low[:, half_ranks:]
    dealt = jnp.concatenate(
        [jnp.broadcast_to(x, (lanes // 2, *x.shape)) for x in (keys, values)], axis=0
    )
    return lax.all_to_all(dealt, LANES, 0, 0, tiled=True).sum(axis=0)


def body(
    hidden,
    key_value_weight,
    adapter_down_weight,
    adapter_up_weight,
    prompt_block_count,
    request_adapter,
    adapter_bank_row,
):
    blocks, block_len, width = hidden.shape
    tokens = blocks * block_len
    owners = lax.axis_size(AA)
    ring = lax.axis_size("ba")
    parity = lax.axis_index("al")
    place = lax.axis_index("ba")
    core = lax.axis_index("col")

    rows = key_value_weight.shape[0]
    half = rows // 2
    kept = lax.dynamic_slice_in_dim(key_value_weight, core * half, half)
    given = lax.dynamic_slice_in_dim(key_value_weight, (1 - core) * half, half)
    weight = jnp.concatenate([kept, lax.ppermute(given, "col", SWAP)], axis=1)
    weight, down, up = lax.optimization_barrier((weight, adapter_down_weight, adapter_up_weight))
    weight = lax.all_gather(weight, "ah", axis=0, tiled=True)

    slots = block_slots(
        prompt_block_count, request_adapter, adapter_bank_row, blocks * owners
    )
    owned, ranks, _ = down.shape
    held = deal_rows(down, up)
    token_rows = hidden.reshape(tokens, width)
    wanted = choose_rows(held, slots, owned)
    own_rows_two = (token_rows, lax.ppermute(token_rows, "col", SWAP))
    pair_rows = exchange(token_rows, 0)

    pair_rows_two = (pair_rows, lax.ppermute(pair_rows, "col", SWAP))
    down_rows, up_rows = own_rows(wanted, blocks, ranks, width)
    low = jnp.einsum("ckf,ctf->ckt", down_rows, hidden, preferred_element_type=jnp.float32)
    active = over_lanes(low)

    ahead = [(2 * i + c, 2 * ((i + 1 - 2 * c) % ring) + c) for i in range(ring) for c in range(2)]
    behind = [(2 * i + c, 2 * ((i - 1 + 2 * c) % ring) + c) for i in range(ring) for c in range(2)]
    turn = 1 - 2 * core
    sources = weight.shape[0] // (half * ring)

    def product(rows_two):
        parts = [
            lax.dot_general(
                weight[:, k * width : (k + 1) * width],
                rows_two[k],
                (((1,), (1,)), ((), ())),
                preferred_element_type=jnp.float32,
            )
            for k in range(2)
        ]
        return (parts[0] + parts[1]).reshape(-1, half, tokens)

    def sums(values):
        def of(target):
            first = sources * lax.rem(target + 2 * ring, ring)
            return lax.dynamic_slice_in_dim(values, first, sources)

        far = lax.ppermute(of(place + 2), LANES, ahead)
        other = lax.ppermute(of(place - turn), LANES, behind)
        near = lax.ppermute(of(place + turn) + far, LANES, ahead)
        return of(place) + other + near

    crossed = exchange(sums(product(pair_rows_two)), 2)
    both = jnp.stack([sums(product(own_rows_two)), crossed])
    both = both.reshape(2, 2, sources // 2, half, tokens)
    here = lax.dynamic_index_in_dim(both, core, 1, keepdims=False)
    there = lax.dynamic_index_in_dim(both, 1 - core, 1, keepdims=False)
    there = lax.ppermute(there, "col", SWAP)
    halves = jnp.stack([jnp.where(core == 0, here, there), jnp.where(core == 0, there, here)])
    even, odd = halves[:, 0], halves[:, 1]
    ordered = jnp.stack([jnp.where(parity == 0, even, odd), jnp.where(parity == 0, odd, even)])
    base = ordered.transpose(2, 0, 1, 3, 4).reshape(-1, tokens).T
    base = base.reshape(blocks, block_len, -1)
    adapted = jnp.einsum(
        "ckt,ckj->ctj", active, up_rows.astype(jnp.float32), precision=lax.Precision.HIGHEST
    )
    return (base + adapted).astype(jnp.bfloat16)


def solution(mesh):
    groups, owners, ring, cores = (mesh.shape[a] for a in ("groups", "aa", "ba", "col"))
    split = Mesh(
        mesh.devices.reshape(groups, owners // 2, 2, ring, cores),
        ("groups", "ah", "al", "ba", "col"),
    )
    rows = ("groups", *AA)
    placed = (
        P(rows, None, LANES),
        P(AA, LANES),
        P(rows, None, LANES),
        P(rows, None, LANES),
        P("groups"),
        P("groups"),
        P("groups"),
    )
    return jax.shard_map(
        body,
        mesh=split,
        in_specs=placed,
        out_specs=P(rows, None, LANES),
        check_vma=False,
    )
```

```python
import jax
import jax.numpy as jnp
from jax import lax
from jax.sharding import Mesh
from jax.sharding import PartitionSpec as P


AA = ("ah", "al")
LANES = ("ba", "col")
SWAP = [(0, 1), (1, 0)]


def block_slots(prompt_block_count, request_adapter, adapter_bank_row, block_total):
    block_ids = jnp.arange(block_total, dtype=jnp.int32)
    requests = prompt_block_count.shape[0]
    earlier = jnp.arange(requests)[:, None] >= jnp.arange(requests)[None, :]
    block_ends = jnp.sum(jnp.where(earlier, prompt_block_count[None, :], 0), axis=1)
    request_of = jnp.sum((block_ends[None, :] <= block_ids[:, None]).astype(jnp.int32), axis=1)
    request_ids = jnp.arange(requests, dtype=jnp.int32)
    adapter_of = jnp.sum(
        jnp.where(request_of[:, None] == request_ids[None, :], request_adapter[None, :], 0), axis=1
    )
    adapter_rows = jnp.arange(adapter_bank_row.shape[0], dtype=jnp.int32)
    return jnp.sum(
        jnp.where(adapter_of[:, None] == adapter_rows[None, :], adapter_bank_row[None, :], 0),
        axis=1,
    )


def exchange(x, axis):
    owners = lax.axis_size(AA)
    up = [(i, (i + 1) % owners) for i in range(owners)]
    down = [(i, (i - 1) % owners) for i in range(owners)]
    first, second = jnp.split(x, 2, axis=axis)
    ways = (up, down) if axis == 0 else (down, up)
    first, second = lax.ppermute(first, AA, ways[0]), lax.ppermute(second, AA, ways[1])
    return jnp.concatenate([first, second], axis=axis)


def across(x):
    owners = lax.axis_size("ah")
    odd = [2 * i + 1 for i in range(owners)]
    even = [2 * ((i + 1) % owners) for i in range(owners)]
    return lax.ppermute(x, AA, [*zip(odd, even), *zip(even, odd)])


def deal_rows(down, up):
    owned, ranks, width = down.shape
    span = up.shape[2]
    halves = ranks // 2
    rest = up.shape[1] * span // ranks
    parity = lax.axis_index("al")
    rows = jnp.concatenate([down, up.reshape(owned, ranks, rest)], axis=2)
    rows = rows.reshape(owned, 2, halves, width + rest)
    kept = lax.dynamic_index_in_dim(rows, parity, 1, keepdims=False)
    given = lax.dynamic_index_in_dim(rows, 1 - parity, 1, keepdims=False)
    rows = jnp.concatenate([kept, across(given)], axis=0)
    owners = lax.axis_size("ah")
    pieces = rows.reshape(2 * owned, owners, -1).transpose(1, 0, 2)
    held = lax.all_to_all(pieces, "ah", 0, 0, tiled=True)
    return held.reshape(owners * 2 * owned, -1)


def choose_rows(held, slots, owned):
    parity = lax.axis_index("al")
    owners = lax.axis_size("ah")
    owner, inside = slots // owned, slots % owned
    step = 1 - 2 * parity
    matching = owner % 2 == parity
    holder = jnp.where(matching, owner // 2, ((owner + step) % (2 * owners)) // 2)
    place = holder * (2 * owned) + jnp.where(matching, inside, inside + owned)
    by_owner = place.reshape(owners, 2, -1)
    own = jnp.where(parity == 0, by_owner[:, 0], by_owner[:, 1])
    other = jnp.where(
        parity == 0, jnp.roll(by_owner[:, 1], 1, axis=0), jnp.roll(by_owner[:, 0], -1, axis=0)
    )
    place = jnp.concatenate([own, other], axis=1).reshape(-1)
    rows = jnp.arange(held.shape[0], dtype=jnp.int32)
    chosen = (place[:, None] == rows[None, :]).astype(held.dtype)
    return jnp.dot(chosen, held, preferred_element_type=jnp.float32).astype(held.dtype)


def own_rows(wanted, blocks, ranks, width):
    parity = lax.axis_index("al")
    owners = lax.axis_size("ah")
    pieces = lax.all_to_all(wanted.reshape(owners, 2 * blocks, -1), "ah", 0, 0, tiled=True)
    kept, taken = pieces[:, :blocks], across(pieces[:, blocks:])
    first = jnp.where(parity == 0, kept, taken)
    second = jnp.where(parity == 0, taken, kept)
    rows = jnp.concatenate([first, second], axis=0).transpose(1, 0, 2)
    rows = rows.reshape(blocks, ranks, -1)
    return rows[:, :, :width], rows[:, :, width:].reshape(blocks, ranks // 2, -1)


def over_lanes(low):
    half_ranks = low.shape[1] // 2
    lanes = lax.axis_size(LANES)
    keys, values = low[:, :half_ranks], low[:, half_ranks:]
    dealt = jnp.concatenate(
        [jnp.broadcast_to(x, (lanes // 2, *x.shape)) for x in (keys, values)], axis=0
    )
    dealt = lax.all_to_all(dealt, LANES, 0, 0, tiled=True)
    return dealt.sum(axis=0)


def body(
    hidden,
    key_value_weight,
    adapter_down_weight,
    adapter_up_weight,
    prompt_block_count,
    request_adapter,
    adapter_bank_row,
):
    blocks, block_len, width = hidden.shape
    tokens = blocks * block_len
    owners = lax.axis_size(AA)
    ring = lax.axis_size("ba")
    parity = lax.axis_index("al")
    place = lax.axis_index("ba")
    core = lax.axis_index("col")

    rows = key_value_weight.shape[0]
    half = rows // 2
    weight = jnp.concatenate(
        [key_value_weight, lax.ppermute(key_value_weight, "col", SWAP)], axis=1
    )
    weight = lax.dynamic_slice_in_dim(weight, core * half, half)
    weight, down, up = lax.optimization_barrier((weight, adapter_down_weight, adapter_up_weight))
    weight = lax.all_gather(weight, "ah", axis=0, tiled=True)

    slots = block_slots(
        prompt_block_count, request_adapter, adapter_bank_row, blocks * owners
    )
    owned, ranks, _ = down.shape
    held = deal_rows(down, up)
    token_rows = hidden.reshape(tokens, width)
    wanted = choose_rows(held, slots, owned)
    own_rows_two = (token_rows, lax.ppermute(token_rows, "col", SWAP))
    pair_rows = exchange(token_rows, 0)

    pair_rows_two = (pair_rows, lax.ppermute(pair_rows, "col", SWAP))
    down_rows, up_rows = own_rows(wanted, blocks, ranks, width)
    low = jnp.einsum("ckf,ctf->ckt", down_rows, hidden, preferred_element_type=jnp.float32)
    active = over_lanes(low)

    ahead = [(2 * i + c, 2 * ((i + 1 - 2 * c) % ring) + c) for i in range(ring) for c in range(2)]
    behind = [(2 * i + c, 2 * ((i - 1 + 2 * c) % ring) + c) for i in range(ring) for c in range(2)]
    turn = 1 - 2 * core
    sources = weight.shape[0] // (half * ring)

    def product(rows_two):
        parts = [
            lax.dot_general(
                weight[:, k * width : (k + 1) * width],
                rows_two[k],
                (((1,), (1,)), ((), ())),
                preferred_element_type=jnp.float32,
            )
            for k in range(2)
        ]
        return (parts[0] + parts[1]).reshape(-1, half, tokens)

    def sums(values):
        def of(target):
            first = sources * lax.rem(target + 2 * ring, ring)
            return lax.dynamic_slice_in_dim(values, first, sources)

        far = lax.ppermute(of(place + 2), LANES, ahead)
        other = lax.ppermute(of(place - turn), LANES, behind)
        near = lax.ppermute(of(place + turn) + far, LANES, ahead)
        return of(place) + other + near

    crossed = exchange(sums(product(pair_rows_two)), 2)
    both = jnp.stack([sums(product(own_rows_two)), crossed])
    both = both.reshape(2, 2, sources // 2, half, tokens)
    here = lax.dynamic_index_in_dim(both, core, 1, keepdims=False)
    there = lax.dynamic_index_in_dim(both, 1 - core, 1, keepdims=False)
    there = lax.ppermute(there, "col", SWAP)
    halves = jnp.stack([jnp.where(core == 0, here, there), jnp.where(core == 0, there, here)])
    even, odd = halves[:, 0], halves[:, 1]
    ordered = jnp.stack([jnp.where(parity == 0, even, odd), jnp.where(parity == 0, odd, even)])
    base = ordered.transpose(2, 0, 1, 3, 4).reshape(-1, tokens).T
    base = base.reshape(blocks, block_len, -1)
    adapted = jnp.einsum(
        "ckt,ckj->ctj", active, up_rows.astype(jnp.float32), precision=lax.Precision.HIGHEST
    )
    return (base + adapted).astype(jnp.bfloat16)


def solution(mesh):
    groups, owners, ring, cores = (mesh.shape[a] for a in ("groups", "aa", "ba", "col"))
    split = Mesh(
        mesh.devices.reshape(groups, owners // 2, 2, ring, cores),
        ("groups", "ah", "al", "ba", "col"),
    )
    rows = ("groups", *AA)
    placed = (
        P(rows, None, LANES),
        P(AA, LANES),
        P(rows, None, LANES),
        P(rows, None, LANES),
        P("groups"),
        P("groups"),
        P("groups"),
    )

    return jax.shard_map(
        body,
        mesh=split,
        in_specs=placed,
        out_specs=P(rows, None, LANES),
        check_vma=False,
    )
```
